32 devices in a mesh: dp: 16 (over z, y, x), mp: 2 (over core).
Axes of the slice: x: 2, y: 2, z: 4, core: 2. Of those that a mesh axis runs over, the one named last changes fastest.
Arguments:
- hidden: bfloat16 [240, 128, 2048], P('dp', None, 'mp'), may hold values from -6 to 6
- attn_out: bfloat16 [240, 128, 2048], P('dp', None, 'mp'), may hold values from -6 to 6
- out_proj: bfloat16 [2048, 2048], P(None, 'mp'), may hold values from -0.125 to 0.125
- norm_gain: float32 [2048], P('mp'), may hold values from 0.1 to 1.9
- reward_proj: float32 [2048, 8], P('mp'), may hold values from -0.125 to 0.125
- block_seq: int32 [240], replicated, may hold values from -1 to 95, as said below
- block_dest: int32 [240], replicated, may hold values from -1 to 159, as said below
- lengths: int32 [96], replicated, may hold values from 1 to 512, as said below
Outputs:
- token_rewards: float32 [160, 8, 128], P('dp')
- advantages: float32 [96], P('dp')
The draws below stay inside these ranges and needn't reach their ends.
Inputs may be any that keep to these rules, and one draw needn't show every extreme that they name: `block_seq`: used slots of each index of dp come first in its 15 slots, the rest hold -1; each index of dp holds 1 to 15 used slots and some index holds exactly 15. Read over used slots in slot order, response numbers never fall, every response appears, and each has 1 to 4 blocks. `block_dest`: exactly the used slots (those of block_seq that are not -1) hold a destination; every owned slot of every owner is named exactly once, so each owner receives exactly 10 blocks; at most 1 block go from one index of dp to one owner, and that many in some pair. `lengths`: A response of n blocks has more than 128 * (n - 1) and at most 128 * n tokens.
All inputs are finite; a program needn't handle non-finite values.
Results may differ from the reference program's by a relative error of at most 0.0029.
Values may be sent and summed in bfloat16 or wider, within the bound.
A program may use at most 64 MiB of HBM per device.

```python
import jax
import jax.numpy as jnp
from jax import lax

D = 2048
HEADS_R = 8
BLK = 128
MOSTB = 4
OWN_CAP = 10
SLOTS_IN = 15
SEQS = 96
BLOCKS_IN = 240
N_DP = 16


def plan_tables(key):
    base = jax.random.fold_in(key, 4242)
    key_busy, key_cells, key_seqs, key_turn, key_owner, key_length = jax.random.split(base, 6)
    key_longest = jax.random.fold_in(base, 7)
    device_count = BLOCKS_IN // SLOTS_IN
    block_total = OWN_CAP * device_count
    busiest = jax.random.randint(key_busy, (), 0, device_count)
    room_left = SLOTS_IN - 1
    extra_blocks = block_total - (device_count - 1) - SLOTS_IN
    cell_order = jax.random.permutation(key_cells, (device_count - 1) * room_left)
    chosen = (cell_order < extra_blocks).astype(jnp.int32).reshape(device_count - 1, room_left).sum(axis=1)
    positions = jnp.arange(device_count, dtype=jnp.int32)
    shifted = jnp.clip(positions - (positions > busiest).astype(jnp.int32), 0, device_count - 2)
    counts = jnp.where(positions == busiest, SLOTS_IN, 1 + chosen[shifted]).astype(jnp.int32)
    starts = jnp.cumsum(counts) - counts
    slot_pos = jnp.arange(SLOTS_IN, dtype=jnp.int32)
    is_used = (slot_pos[None, :] < counts[:, None]).reshape(-1)
    global_pos = (starts[:, None] + slot_pos[None, :]).reshape(-1)
    global_pos = jnp.where(is_used, global_pos, 0)
    seq_extra = block_total - SEQS
    cell_total = SEQS * (MOSTB - 1)
    longest = jax.random.randint(key_longest, (), 0, SEQS)
    seq_cells = jax.random.permutation(key_seqs, cell_total).astype(jnp.int32)
    cell_index = jnp.arange(cell_total, dtype=jnp.int32)
    cell_row = cell_index // (MOSTB - 1)
    sort_keys = jnp.where(cell_row == longest, -1 - cell_index % (MOSTB - 1), seq_cells)
    cell_rank = jnp.argsort(jnp.argsort(sort_keys, stable=True), stable=True).astype(jnp.int32)
    seq_blocks = 1 + (cell_rank < seq_extra).astype(jnp.int32).reshape(SEQS, MOSTB - 1).sum(axis=1)
    seq_starts = jnp.cumsum(seq_blocks) - seq_blocks
    seq_of = (seq_starts[None, :] <= global_pos[:, None]).astype(jnp.int32).sum(axis=1) - 1
    block_seq = jnp.where(is_used, seq_of, -1)
    rotation = jax.random.randint(key_turn, (), 0, device_count)
    owner_order = jax.random.permutation(key_owner, device_count)
    owner_rank = owner_order[(global_pos + rotation) % device_count]
    destination = jnp.where(is_used, owner_rank * OWN_CAP + global_pos // device_count, -1)
    tail_tokens = jax.random.randint(key_length, (SEQS,), 1, BLK + 1)
    seq_ids = jnp.arange(SEQS, dtype=jnp.int32)
    tail_tokens = jnp.where(seq_ids == longest, BLK, tail_tokens)
    lengths = BLK * (seq_blocks - 1) + tail_tokens
    return (block_seq.astype(jnp.int32), destination.astype(jnp.int32), lengths.astype(jnp.int32))


def draw_block_seq(key, part):
    return plan_tables(key)[0]


def draw_block_dest(key, part):
    return plan_tables(key)[1]


def draw_lengths(key, part):
    return plan_tables(key)[2]


def shard_levels(key, dims, shards, least, largest):
    loudness, own = 1.0, jax.random.fold_in(key, 6)
    for axis_at, shards_of in shards:
        heights = jnp.exp(jax.random.uniform(jax.random.fold_in(own, axis_at), (shards_of,), jnp.float32, least / len(shards), largest / len(shards)))
        loudness = loudness * jnp.repeat(heights, dims[axis_at] // shards_of).reshape([-1 if axis == axis_at else 1 for axis in range(len(dims))])
    return loudness


def centred(rng, dims, scale, reach, pieces=(), kind=jnp.bfloat16):
    loudness = shard_levels(rng, dims, pieces, -0.22, 0.18) if pieces else 1.0
    entries = jax.random.normal(rng, dims, jnp.float32) * scale * loudness
    return jnp.minimum(jnp.maximum(entries, -reach), reach).astype(kind)


def setup_inputs(seed: int = 0) -> dict:
    arg_keys = jax.random.split(jax.random.key(seed), 9)
    return {
        "hidden": centred(arg_keys[0], (BLOCKS_IN, BLK, D), 1.0, 6.0, ((0, 16), (2, 2))),
        "attn_out": centred(arg_keys[1], (BLOCKS_IN, BLK, D), 1.0, 6.0, ((0, 16), (2, 2))),
        "out_proj": centred(arg_keys[2], (D, D), D ** -0.5, 0.125, ((1, 2),)),
        "norm_gain": jnp.clip(1.0 + 0.18 * jax.random.normal(arg_keys[3], (D,), jnp.float32), 0.1, 1.9),
        "reward_proj": centred(arg_keys[4], (D, HEADS_R), D ** -0.5, 0.125, ((0, 2),), jnp.float32),
        "block_seq": draw_block_seq(jax.random.fold_in(arg_keys[8], 71), 0),
        "block_dest": draw_block_dest(jax.random.fold_in(arg_keys[8], 71), 0),
        "lengths": draw_lengths(jax.random.fold_in(arg_keys[8], 71), 0),
    }


norm_epsilon = 1e-05
stat_epsilon = 1e-06

def reference(hidden, attn_out, out_proj, norm_gain, reward_proj, block_seq, block_dest, lengths):
    slot_count = block_seq.shape[0]
    owned_count = OWN_CAP * N_DP
    slot_index = jnp.arange(slot_count, dtype=jnp.int32)
    is_used = block_dest >= 0
    target = jnp.where(is_used, block_dest, owned_count).astype(jnp.int32)
    source = jnp.zeros((owned_count,), jnp.int32).at[target].set(slot_index, mode='drop')
    seq_safe = jnp.where(is_used, block_seq, 0).astype(jnp.int32)
    used_int = is_used.astype(jnp.int32)
    per_seq = jnp.zeros((SEQS,), jnp.int32).at[seq_safe].add(used_int)
    seq_starts = jnp.cumsum(per_seq) - per_seq
    global_pos = jnp.cumsum(used_int) - 1
    seq_rank = global_pos - seq_starts[seq_safe]
    valid_tokens = jnp.minimum(BLK, lengths[seq_safe] - BLK * seq_rank)
    src_seq = seq_safe[source]
    src_valid = valid_tokens[source]

    def one_block(slot):
        projected = jnp.dot(attn_out[slot], out_proj, preferred_element_type=jnp.float32)
        stored = (hidden[slot].astype(jnp.float32) + projected).astype(jnp.bfloat16)
        stored = lax.optimization_barrier(stored)
        values = stored.astype(jnp.float32)
        mean_sq = lax.optimization_barrier(jnp.mean(values * values, axis=1, keepdims=True))
        normed = values * lax.rsqrt(mean_sq + norm_epsilon) * norm_gain[None, :]
        return jnp.dot(normed, reward_proj, precision=lax.Precision.HIGHEST)
    rewards = lax.map(one_block, source)
    live = jnp.arange(BLK, dtype=jnp.int32)[None, :] < src_valid[:, None]
    rewards = jnp.where(live[:, :, None], rewards, jnp.float32(0.0))
    token_rewards = jnp.transpose(rewards, (0, 2, 1))
    block_sums = lax.optimization_barrier(jnp.sum(token_rewards, axis=2))
    seq_totals = jnp.zeros((SEQS, HEADS_R), jnp.float32).at[src_seq].add(block_sums)
    scores = seq_totals / lengths[:, None].astype(jnp.float32)
    worst_case = lax.optimization_barrier(jnp.min(scores, axis=1))
    head_mean = lax.optimization_barrier(jnp.mean(scores, axis=1))
    spread = lax.optimization_barrier(jnp.mean((scores - head_mean[:, None]) ** 2, axis=1))
    penalty_scale = jnp.mean(spread) + stat_epsilon
    conservative = worst_case - spread / penalty_scale
    centre = jnp.mean(conservative)
    variance = jnp.mean((conservative - centre) ** 2)
    advantages = (conservative - centre) / jnp.sqrt(variance + stat_epsilon)
    return (token_rewards, advantages)
```

```python
import functools

import jax
import jax.numpy as jnp
from jax import lax
from jax.experimental import pallas as pl
from jax.experimental.pallas import tpu as pltpu
from jax.sharding import PartitionSpec as P

OWN_CAP = 10

norm_epsilon = 1e-05
stat_epsilon = 1e-06
MESH = pl.DeviceIdType.MESH
LANES = 128


def split_size(slots):
    for size in (3, 4, 2, 5):
        if slots % size == 0:
            return size
    return 1


def kernel(
    n_dp, n_mp, slots, block_len, seq_count, per_group,
    hidden_hbm, attn_hbm, w_hbm, gain_ref, reward_ref, seq_s, dest_s, len_s, seq_v, dest_v, len_v,
    rewards_out, adv_out,
    attn, w, hidden, acc, resid, heads_w, part, live, rewards, seq_acc, send_buf, recv_buf, adv_buf,
    send_idx, recv_idx,
    w_sem, own_sem, hid_sem, attn_send, attn_recv, part_send, part_recv, dp_send, dp_recv,
):
    dp = lax.axis_index("dp")
    mp = lax.axis_index("mp")
    groups = slots // per_group
    rows = per_group * block_len
    k_local = attn_hbm.shape[1]
    n_local = w_hbm.shape[1]
    model_width = w_hbm.shape[0]
    chunk = min(256, n_local)
    n_chunks = n_local // chunk

    barrier = pltpu.get_barrier_semaphore()
    for off in range(1, n_mp):
        pl.semaphore_signal(barrier, inc=1, device_id=(dp, lax.rem(mp + off, n_mp)), device_id_type=MESH)
    for off in range(1, n_dp):
        pl.semaphore_signal(barrier, inc=1, device_id=(lax.rem(dp + off, n_dp), mp), device_id_type=MESH)

    def w_copy(m):
        start = pl.multiple_of(m * k_local, k_local)
        return pltpu.make_async_copy(w_hbm.at[pl.ds(start, k_local)], w.at[m], w_sem.at[m])

    def group_rows(g):
        return pl.ds(pl.multiple_of(g * rows, rows), rows)

    def own_copy(g):
        return pltpu.make_async_copy(attn_hbm.at[group_rows(g)], attn.at[mp, group_rows(g)], own_sem.at[g])

    def hid_copy(g):
        return pltpu.make_async_copy(hidden_hbm.at[group_rows(g)], hidden.at[group_rows(g)], hid_sem.at[g])

    def attn_copy(off, g):
        return pltpu.make_async_remote_copy(
            src_ref=attn_hbm.at[group_rows(g)],
            dst_ref=attn.at[mp, group_rows(g)],
            send_sem=attn_send.at[off - 1, g],
            recv_sem=attn_recv.at[off - 1, g],
            device_id=(dp, lax.rem(mp + off, n_mp)),
            device_id_type=MESH,
        )

    def part_copy(off, g):
        return pltpu.make_async_remote_copy(
            src_ref=part.at[mp, g],
            dst_ref=part.at[mp, g],
            send_sem=part_send.at[off - 1, g],
            recv_sem=part_recv.at[off - 1, g],
            device_id=(dp, lax.rem(mp + off, n_mp)),
            device_id_type=MESH,
        )

    def dp_copy(off):
        peer = lax.rem(dp + off, n_dp)
        return pltpu.make_async_remote_copy(
            src_ref=send_buf.at[peer],
            dst_ref=recv_buf.at[dp],
            send_sem=dp_send.at[off - 1],
            recv_sem=dp_recv.at[off - 1],
            device_id=(peer, mp),
            device_id_type=MESH,
        )

    w_copy(mp).start()
    for g in range(groups):
        own_copy(g).start()
    for off in range(1, n_mp):
        w_copy(lax.rem(mp + off, n_mp)).start()
    for g in range(groups):
        hid_copy(g).start()

    head_count = reward_ref.shape[0]
    weighted = reward_ref[...] * gain_ref[...].reshape(1, n_local)
    high = weighted.astype(jnp.bfloat16)
    rest = weighted - high.astype(jnp.float32)
    middle = rest.astype(jnp.bfloat16)
    low = (rest - middle.astype(jnp.float32)).astype(jnp.bfloat16)
    heads_w[...] = jnp.concatenate([high, middle, low, jnp.zeros_like(low)], axis=0)

    base = dp * slots

    def send_body(r, carry):
        low_dest = r * OWN_CAP
        found = jnp.int32(0)
        for j in range(slots):
            d = dest_s[base + j]
            found = jnp.where((d >= low_dest) & (d < low_dest + OWN_CAP), jnp.int32(j), found)
        send_idx[r] = found
        return carry

    lax.fori_loop(0, n_dp, send_body, 0)
    all_slots = seq_s.shape[0]
    slot_lane = lax.broadcasted_iota(jnp.int32, (1, all_slots), 1)
    dest_row = dest_v[...].reshape(1, all_slots)
    seq_row = seq_v[...].reshape(1, all_slots)
    for q in range(OWN_CAP):
        place = jnp.max(jnp.where(dest_row == dp * OWN_CAP + q, slot_lane, 0))
        recv_idx[q] = lax.div(place, slots)
    token = lax.broadcasted_iota(jnp.int32, (1, block_len), 1).astype(jnp.float32)
    for j in range(slots):
        seq = seq_s[base + j]
        earlier = jnp.where((seq_row == seq) & (slot_lane < base + j), 1.0, 0.0)
        rank = jnp.sum(earlier, axis=1, keepdims=True)
        length = len_s[jnp.maximum(seq, 0)].astype(jnp.float32)
        valid = length - rank * float(block_len)
        live[j : j + 1, :] = jnp.where(token < valid, 1.0, 0.0)
    seq_acc[...] = jnp.zeros_like(seq_acc)

    pl.semaphore_wait(barrier, n_mp - 1 + n_dp - 1)
    for g in range(groups):
        for off in range(1, n_mp):
            attn_copy(off, g).start()

    w_copy(mp).wait()

    def first_half(g, carry):
        own_copy(g).wait()
        for c in range(n_chunks):
            cols = slice(c * chunk, (c + 1) * chunk)
            acc[group_rows(g), cols] = jnp.dot(
                attn[mp, group_rows(g), :], w[mp, :, cols], preferred_element_type=jnp.float32
            )
        return carry

    lax.fori_loop(0, groups, first_half, 0)
    for off in range(1, n_mp):
        w_copy(lax.rem(mp + off, n_mp)).wait()

    seq_lane = lax.broadcasted_iota(jnp.int32, (head_count, seq_acc.shape[1]), 1)

    def finish(g):
        for off in range(1, n_mp):
            part_copy(off, g).wait()
        total = part[0, g]
        for m in range(1, n_mp):
            total = total + part[m, g]
        scale = lax.rsqrt(total[head_count:] / model_width + norm_epsilon)
        values = total[:head_count] * scale
        for b in range(per_group):
            j = g * per_group + b
            block = values[:, b * block_len : (b + 1) * block_len] * live[pl.ds(j, 1), :]
            rewards[j] = block
            sums = jnp.sum(block, axis=1, keepdims=True)
            seq_acc[...] += jnp.where(seq_lane == seq_s[base + j], sums, 0.0)

    def second_half(g, carry):
        hid_copy(g).wait()
        for off in range(1, n_mp):
            attn_copy(off, g).wait()
        squares = jnp.zeros((rows, LANES), jnp.float32)
        for c in range(n_chunks):
            cols = slice(c * chunk, (c + 1) * chunk)
            total = acc[group_rows(g), cols]
            for off in range(1, n_mp):
                m = lax.rem(mp + off, n_mp)
                total = total + jnp.dot(
                    attn[m, group_rows(g), :], w[m, :, cols], preferred_element_type=jnp.float32
                )
            stored = (hidden[group_rows(g), cols].astype(jnp.float32) + total).astype(jnp.bfloat16)
            resid[:, cols] = stored
            v = stored.astype(jnp.float32)
            for i in range(chunk // LANES):
                piece = v[:, i * LANES : (i + 1) * LANES]
                squares = squares + piece * piece
        heads = lax.dot_general(
            heads_w[...], resid[...], (((1,), (1,)), ((), ())), preferred_element_type=jnp.float32
        )
        h = head_count
        part[mp, g, 0:h, :] = heads[0:h] + heads[h : 2 * h] + heads[2 * h : 3 * h]
        sum_row = jnp.sum(jnp.transpose(squares), axis=0, keepdims=True)
        part[mp, g, h : 2 * h, :] = jnp.broadcast_to(sum_row, (h, rows))
        for off in range(1, n_mp):
            part_copy(off, g).start()

        @pl.when(g > 0)
        def _():
            finish(g - 1)

        return carry

    lax.fori_loop(0, groups, second_half, 0)
    finish(groups - 1)

    seq_part = seq_acc[...]

    def fill(r, carry):
        send_buf[r, :, 0:block_len] = rewards[send_idx[r]]
        send_buf[r, :, block_len:] = seq_part
        return carry

    lax.fori_loop(0, n_dp, fill, 0, unroll=n_dp <= 16)
    recv_buf[dp] = send_buf[dp]
    for off in range(1, n_dp):
        dp_copy(off).start()
    for off in range(1, n_dp):
        dp_copy(off).wait()
    for q in range(OWN_CAP):
        rewards_out[q] = recv_buf[recv_idx[q], :, 0:block_len]
    totals = recv_buf[0, :, block_len:]
    for s in range(1, n_dp):
        totals = totals + recv_buf[s, :, block_len:]
    scores = totals[:, :seq_count] / len_v[...].reshape(1, seq_count).astype(jnp.float32)
    worst = jnp.min(scores, axis=0, keepdims=True)
    centred = scores - jnp.mean(scores, axis=0, keepdims=True)
    spread = jnp.mean(centred * centred, axis=0, keepdims=True)
    penalty_scale = jnp.mean(spread, axis=1, keepdims=True) + stat_epsilon
    conservative = worst - spread / penalty_scale
    shifted = conservative - jnp.mean(conservative, axis=1, keepdims=True)
    variance = jnp.mean(shifted * shifted, axis=1, keepdims=True)
    adv_buf[...] = jnp.zeros_like(adv_buf)
    adv_buf[0:1, :seq_count] = shifted * lax.rsqrt(variance + stat_epsilon)
    width = adv_buf.shape[1]
    seq_local = adv_out.shape[1]
    turned = pltpu.roll(adv_buf[...], width - dp * seq_local, 1)
    adv_out[...] = turned[0:1, :seq_local]


def local(n_dp, n_mp, hidden, attn_out, out_proj, norm_gain, reward_proj, block_seq, block_dest, lengths):
    slots, block_len, k_local = attn_out.shape
    n_local = out_proj.shape[1]
    seq_count = lengths.shape[0]
    seq_pad = -(-seq_count // LANES) * LANES
    heads = reward_proj.shape[1]
    per_group = split_size(slots)
    groups = slots // per_group
    rows = per_group * block_len
    total_rows = slots * block_len
    f32, bf16 = jnp.float32, jnp.bfloat16
    dma = pltpu.SemaphoreType.DMA
    any_spec = pl.BlockSpec(memory_space=pl.ANY)
    vmem_spec = pl.BlockSpec(memory_space=pltpu.VMEM)
    smem_spec = pl.BlockSpec(memory_space=pltpu.SMEM)
    token_rewards, advantages = pl.pallas_call(
        functools.partial(kernel, n_dp, n_mp, slots, block_len, seq_count, per_group),
        out_shape=(
            jax.ShapeDtypeStruct((OWN_CAP, heads, block_len), f32),
            jax.ShapeDtypeStruct((1, seq_count // n_dp), f32),
        ),
        in_specs=[any_spec] * 3 + [vmem_spec] * 2 + [smem_spec] * 3 + [vmem_spec] * 3,
        out_specs=(vmem_spec, vmem_spec),
        scratch_shapes=[
            pltpu.VMEM((n_mp, total_rows, k_local), bf16),
            pltpu.VMEM((n_mp, k_local, n_local), bf16),
            pltpu.VMEM((total_rows, n_local), bf16),
            pltpu.VMEM((total_rows, n_local), f32),
            pltpu.VMEM((rows, n_local), bf16),
            pltpu.VMEM((4 * heads, n_local), bf16),
            pltpu.VMEM((n_mp, groups, 2 * heads, rows), f32),
            pltpu.VMEM((slots + (-slots) % 8, block_len), f32),
            pltpu.VMEM((slots, heads, block_len), f32),
            pltpu.VMEM((heads, seq_pad), f32),
            pltpu.VMEM((n_dp, heads, block_len + seq_pad), f32),
            pltpu.VMEM((n_dp, heads, block_len + seq_pad), f32),
            pltpu.VMEM((8, seq_pad), f32),
            pltpu.SMEM((n_dp,), jnp.int32),
            pltpu.SMEM((OWN_CAP,), jnp.int32),
            dma((n_mp,)),
            dma((groups,)),
            dma((groups,)),
            dma((n_mp - 1, groups)),
            dma((n_mp - 1, groups)),
            dma((n_mp - 1, groups)),
            dma((n_mp - 1, groups)),
            dma((n_dp - 1,)),
            dma((n_dp - 1,)),
        ],
        compiler_params=pltpu.CompilerParams(
            collective_id=0, has_side_effects=True, vmem_limit_bytes=60 * 1024 * 1024
        ),
    )(
        hidden.reshape(total_rows, n_local),
        attn_out.reshape(total_rows, k_local),
        out_proj,
        norm_gain,
        reward_proj.T,
        block_seq,
        block_dest,
        lengths,
        block_seq,
        block_dest,
        lengths,
    )
    return token_rewards, advantages.reshape(seq_count // n_dp)


def solution(mesh):
    return jax.shard_map(
        functools.partial(local, mesh.shape["dp"], mesh.shape["mp"]),
        mesh=mesh,
        in_specs=(
            P("dp", None, "mp"),
            P("dp", None, "mp"),
            P(None, "mp"),
            P("mp"),
            P("mp", None),
            P(),
            P(),
            P(),
        ),
        out_specs=(P("dp", None, None), P("dp")),
        check_vma=False,
    )
```

```python
import functools

import jax
import jax.numpy as jnp
from jax import lax
from jax.experimental import pallas as pl
from jax.experimental.pallas import tpu as pltpu
from jax.sharding import PartitionSpec as P

OWN_CAP = 10

norm_epsilon = 1e-05
stat_epsilon = 1e-06
MESH = pl.DeviceIdType.MESH
LANES = 128


def split_size(slots):
    for size in (5, 4, 3, 2):
        if slots % size == 0:
            return size
    return 1


def kernel(
    n_dp, n_mp, slots, block_len, seq_count, per_group,
    hidden_hbm, attn_hbm, w_hbm, gain_hbm, reward_hbm, seq_hbm, dest_hbm, len_hbm,
    recv_buf,
    attn, w, hidden, acc, resid, heads_w, part, live, rewards, seq_acc, send_buf,
    send_idx, gain_ref, reward_ref, seq_s, dest_s, len_s, seq_v, small_sem,
    w_sem, own_sem, hid_sem, attn_send, attn_recv, part_send, part_recv, dp_send, dp_recv,
):
    dp = lax.axis_index("dp")
    mp = lax.axis_index("mp")
    groups = slots // per_group
    rows = per_group * block_len
    k_local = attn_hbm.shape[1]
    n_local = w_hbm.shape[1]
    model_width = w_hbm.shape[0]
    chunk = min(256, n_local)
    n_chunks = n_local // chunk

    barrier = pltpu.get_barrier_semaphore()
    for off in range(1, n_mp):
        pl.semaphore_signal(barrier, inc=1, device_id=(dp, lax.rem(mp + off, n_mp)), device_id_type=MESH)
    for off in range(1, n_dp):
        pl.semaphore_signal(barrier, inc=1, device_id=(lax.rem(dp + off, n_dp), mp), device_id_type=MESH)

    def w_copy(m):
        start = pl.multiple_of(m * k_local, k_local)
        return pltpu.make_async_copy(w_hbm.at[pl.ds(start, k_local)], w.at[m], w_sem.at[m])

    def group_rows(g):
        return pl.ds(pl.multiple_of(g * rows, rows), rows)

    def own_copy(g):
        return pltpu.make_async_copy(attn_hbm.at[group_rows(g)], attn.at[mp, group_rows(g)], own_sem.at[g])

    def hid_copy(g):
        return pltpu.make_async_copy(hidden_hbm.at[group_rows(g)], hidden.at[group_rows(g)], hid_sem.at[g])

    def attn_copy(off, g):
        return pltpu.make_async_remote_copy(
            src_ref=attn_hbm.at[group_rows(g)],
            dst_ref=attn.at[mp, group_rows(g)],
            send_sem=attn_send.at[off - 1, g],
            recv_sem=attn_recv.at[off - 1, g],
            device_id=(dp, lax.rem(mp + off, n_mp)),
            device_id_type=MESH,
        )

    def part_copy(off, g):
        return pltpu.make_async_remote_copy(
            src_ref=part.at[mp, g],
            dst_ref=part.at[mp, g],
            send_sem=part_send.at[off - 1, g],
            recv_sem=part_recv.at[off - 1, g],
            device_id=(dp, lax.rem(mp + off, n_mp)),
            device_id_type=MESH,
        )

    def dp_copy(off):
        peer = lax.rem(dp + off, n_dp)
        return pltpu.make_async_remote_copy(
            src_ref=send_buf.at[peer],
            dst_ref=recv_buf.at[dp],
            send_sem=dp_send.at[off - 1],
            recv_sem=dp_recv.at[off - 1],
            device_id=(peer, mp),
            device_id_type=MESH,
        )

    small = [
        pltpu.make_async_copy(src, dst, small_sem.at[i])
        for i, (src, dst) in enumerate(
            (
                (gain_hbm, gain_ref),
                (reward_hbm, reward_ref),
                (seq_hbm, seq_s),
                (dest_hbm, dest_s),
                (len_hbm, len_s),
                (seq_hbm, seq_v),
            )
        )
    ]
    for copy in small:
        copy.start()
    w_copy(mp).start()
    for g in range(groups):
        own_copy(g).start()
    for off in range(1, n_mp):
        w_copy(lax.rem(mp + off, n_mp)).start()
    for g in range(groups):
        hid_copy(g).start()

    for copy in small:
        copy.wait()
    head_count = reward_ref.shape[0]
    weighted = reward_ref[...] * gain_ref[...].reshape(1, n_local)
    high = weighted.astype(jnp.bfloat16)
    rest = weighted - high.astype(jnp.float32)
    middle = rest.astype(jnp.bfloat16)
    low = (rest - middle.astype(jnp.float32)).astype(jnp.bfloat16)
    heads_w[...] = jnp.concatenate([high, middle, low, jnp.zeros_like(low)], axis=0)

    base = dp * slots

    def send_body(r, carry):
        low_dest = r * OWN_CAP
        found = jnp.int32(0)
        for j in range(slots):
            d = dest_s[base + j]
            found = jnp.where((d >= low_dest) & (d < low_dest + OWN_CAP), jnp.int32(j), found)
        send_idx[r] = found
        return carry

    lax.fori_loop(0, n_dp, send_body, 0)
    all_slots = seq_s.shape[0]
    slot_lane = lax.broadcasted_iota(jnp.int32, (1, all_slots), 1)
    seq_row = seq_v[...].reshape(1, all_slots)
    token = lax.broadcasted_iota(jnp.int32, (1, block_len), 1).astype(jnp.float32)
    for j in range(slots):
        seq = seq_s[base + j]
        earlier = jnp.where((seq_row == seq) & (slot_lane < base + j), 1.0, 0.0)
        rank = jnp.sum(earlier, axis=1, keepdims=True)
        length = len_s[jnp.maximum(seq, 0)].astype(jnp.float32)
        valid = length - rank * float(block_len)
        live[j : j + 1, :] = jnp.where(token < valid, 1.0, 0.0)
    seq_acc[...] = jnp.zeros_like(seq_acc)

    pl.semaphore_wait(barrier, n_mp - 1 + n_dp - 1)
    for g in range(groups):
        for off in range(1, n_mp):
            attn_copy(off, g).start()

    w_copy(mp).wait()

    def first_half(g, carry):
        own_copy(g).wait()
        for c in range(n_chunks):
            cols = slice(c * chunk, (c + 1) * chunk)
            acc[group_rows(g), cols] = jnp.dot(
                attn[mp, group_rows(g), :], w[mp, :, cols], preferred_element_type=jnp.float32
            )
        return carry

    lax.fori_loop(0, groups, first_half, 0)
    for off in range(1, n_mp):
        w_copy(lax.rem(mp + off, n_mp)).wait()

    seq_lane = lax.broadcasted_iota(jnp.int32, (head_count, seq_acc.shape[1]), 1)

    def finish(g):
        for off in range(1, n_mp):
            part_copy(off, g).wait()
        total = part[0, g]
        for m in range(1, n_mp):
            total = total + part[m, g]
        scale = lax.rsqrt(total[head_count:] / model_width + norm_epsilon)
        values = total[:head_count] * scale
        for b in range(per_group):
            j = g * per_group + b
            block = values[:, b * block_len : (b + 1) * block_len] * live[pl.ds(j, 1), :]
            rewards[j] = block
            sums = jnp.sum(block, axis=1, keepdims=True)
            seq_acc[...] += jnp.where(seq_lane == seq_s[base + j], sums, 0.0)

    def second_half(g, carry):
        hid_copy(g).wait()
        for off in range(1, n_mp):
            attn_copy(off, g).wait()
        squares = jnp.zeros((rows, LANES), jnp.float32)
        for c in range(n_chunks):
            cols = slice(c * chunk, (c + 1) * chunk)
            total = acc[group_rows(g), cols]
            for off in range(1, n_mp):
                m = lax.rem(mp + off, n_mp)
                total = total + jnp.dot(
                    attn[m, group_rows(g), :], w[m, :, cols], preferred_element_type=jnp.float32
                )
            stored = (hidden[group_rows(g), cols].astype(jnp.float32) + total).astype(jnp.bfloat16)
            resid[:, cols] = stored
            v = stored.astype(jnp.float32)
            for i in range(chunk // LANES):
                piece = v[:, i * LANES : (i + 1) * LANES]
                squares = squares + piece * piece
        heads = lax.dot_general(
            heads_w[...], resid[...], (((1,), (1,)), ((), ())), preferred_element_type=jnp.float32
        )
        h = head_count
        part[mp, g, 0:h, :] = heads[0:h] + heads[h : 2 * h] + heads[2 * h : 3 * h]
        sum_row = jnp.sum(jnp.transpose(squares), axis=0, keepdims=True)
        part[mp, g, h : 2 * h, :] = jnp.broadcast_to(sum_row, (h, rows))
        for off in range(1, n_mp):
            part_copy(off, g).start()

        @pl.when(g > 0)
        def _():
            finish(g - 1)

        return carry

    lax.fori_loop(0, groups, second_half, 0)
    finish(groups - 1)

    seq_part = seq_acc[...]

    def fill(r, carry):
        send_buf[r, :, 0:block_len] = rewards[send_idx[r]]
        send_buf[r, :, block_len:] = seq_part
        return carry

    lax.fori_loop(0, n_dp, fill, 0, unroll=n_dp <= 16)
    kept = pltpu.make_async_copy(send_buf.at[dp], recv_buf.at[dp], small_sem.at[0])
    kept.start()
    for off in range(1, n_dp):
        dp_copy(off).start()
    for off in range(1, n_dp):
        dp_copy(off).wait()
    kept.wait()


def finish_kernel(n_dp, slots, seq_count, block_len, recv_buf, dest_v, len_v, rewards_out, adv_out, adv_buf):
    dp = lax.axis_index("dp")
    all_slots = dest_v.shape[0]
    slot_lane = lax.broadcasted_iota(jnp.int32, (1, all_slots), 1)
    dest_row = dest_v[...].reshape(1, all_slots)
    for q in range(OWN_CAP):
        place = jnp.max(jnp.where(dest_row == dp * OWN_CAP + q, slot_lane, 0))
        rewards_out[q] = recv_buf[lax.div(place, slots), :, 0:block_len]
    totals = recv_buf[0, :, block_len:]
    for s in range(1, n_dp):
        totals = totals + recv_buf[s, :, block_len:]
    scores = totals[:, :seq_count] / len_v[...].reshape(1, seq_count).astype(jnp.float32)
    worst = jnp.min(scores, axis=0, keepdims=True)
    centred = scores - jnp.mean(scores, axis=0, keepdims=True)
    spread = jnp.mean(centred * centred, axis=0, keepdims=True)
    penalty_scale = jnp.mean(spread, axis=1, keepdims=True) + stat_epsilon
    conservative = worst - spread / penalty_scale
    shifted = conservative - jnp.mean(conservative, axis=1, keepdims=True)
    variance = jnp.mean(shifted * shifted, axis=1, keepdims=True)
    adv_buf[...] = jnp.zeros_like(adv_buf)
    adv_buf[0:1, :seq_count] = shifted * lax.rsqrt(variance + stat_epsilon)
    width = adv_buf.shape[1]
    seq_local = adv_out.shape[1]
    turned = pltpu.roll(adv_buf[...], width - dp * seq_local, 1)
    adv_out[...] = turned[0:1, :seq_local]

def local(n_dp, n_mp, hidden, attn_out, out_proj, norm_gain, reward_proj, block_seq, block_dest, lengths):
    slots, block_len, k_local = attn_out.shape
    n_local = out_proj.shape[1]
    seq_count = lengths.shape[0]
    seq_pad = -(-seq_count // LANES) * LANES
    heads = reward_proj.shape[1]
    per_group = split_size(slots)
    groups = slots // per_group
    rows = per_group * block_len
    total_rows = slots * block_len
    f32, bf16 = jnp.float32, jnp.bfloat16
    dma = pltpu.SemaphoreType.DMA
    any_spec = pl.BlockSpec(memory_space=pl.ANY)
    vmem_spec = pl.BlockSpec(memory_space=pltpu.VMEM)
    width = block_len + seq_pad
    received = pl.pallas_call(
        functools.partial(kernel, n_dp, n_mp, slots, block_len, seq_count, per_group),
        out_shape=jax.ShapeDtypeStruct((n_dp, heads, width), f32),
        in_specs=[any_spec] * 8,
        out_specs=any_spec,
        scratch_shapes=[
            pltpu.VMEM((n_mp, total_rows, k_local), bf16),
            pltpu.VMEM((n_mp, k_local, n_local), bf16),
            pltpu.VMEM((total_rows, n_local), bf16),
            pltpu.VMEM((total_rows, n_local), f32),
            pltpu.VMEM((rows, n_local), bf16),
            pltpu.VMEM((4 * heads, n_local), bf16),
            pltpu.VMEM((n_mp, groups, 2 * heads, rows), f32),
            pltpu.VMEM((slots + (-slots) % 8, block_len), f32),
            pltpu.VMEM((slots, heads, block_len), f32),
            pltpu.VMEM((heads, seq_pad), f32),
            pltpu.VMEM((n_dp, heads, width), f32),
            pltpu.SMEM((n_dp,), jnp.int32),
            pltpu.VMEM(norm_gain.shape, f32),
            pltpu.VMEM((heads, n_local), f32),
            pltpu.SMEM(block_seq.shape, jnp.int32),
            pltpu.SMEM(block_dest.shape, jnp.int32),
            pltpu.SMEM(lengths.shape, jnp.int32),
            pltpu.VMEM(block_seq.shape, jnp.int32),
            dma((6,)),
            dma((n_mp,)),
            dma((groups,)),
            dma((groups,)),
            dma((n_mp - 1, groups)),
            dma((n_mp - 1, groups)),
            dma((n_mp - 1, groups)),
            dma((n_mp - 1, groups)),
            dma((n_dp - 1,)),
            dma((n_dp - 1,)),
        ],
        compiler_params=pltpu.CompilerParams(
            collective_id=0, has_side_effects=True, vmem_limit_bytes=60 * 1024 * 1024
        ),
    )(
        hidden.reshape(total_rows, n_local),
        attn_out.reshape(total_rows, k_local),
        out_proj,
        norm_gain,
        reward_proj.T,
        block_seq,
        block_dest,
        lengths,
    )
    token_rewards, advantages = pl.pallas_call(
        functools.partial(finish_kernel, n_dp, slots, seq_count, block_len),
        out_shape=(
            jax.ShapeDtypeStruct((OWN_CAP, heads, block_len), f32),
            jax.ShapeDtypeStruct((1, seq_count // n_dp), f32),
        ),
        in_specs=[vmem_spec] * 3,
        out_specs=(vmem_spec, vmem_spec),
        scratch_shapes=[pltpu.VMEM((8, seq_pad), f32)],
    )(received, block_dest, lengths)
    return token_rewards, advantages.reshape(seq_count // n_dp)


def solution(mesh):
    return jax.shard_map(
        functools.partial(local, mesh.shape["dp"], mesh.shape["mp"]),
        mesh=mesh,
        in_specs=(
            P("dp", None, "mp"),
            P("dp", None, "mp"),
            P(None, "mp"),
            P("mp"),
            P("mp", None),
            P(),
            P(),
            P(),
        ),
        out_specs=(P("dp", None, None), P("dp")),
        check_vma=False,
    )
```
